8 devices in a mesh: fit: 1 (over z), comp: 2 (over y), pts: 4 (over x, core).
Axes of the slice: x: 2, y: 2, z: 1, core: 2. Of those that a mesh axis runs over, the one named last changes fastest.
Arguments:
- points: bfloat16 [2048, 128], P(('fit', 'pts'))
- means_init: float32 [65536, 128], P(('fit', 'comp'))
- logw_init: float32 [65536], P(('fit', 'comp'))
- inv_temp: float32 [3], replicated
Outputs:
- output 1: float32 [65536, 128], P(('fit', 'comp'))
- output 2: float32 [65536], P(('fit', 'comp'))
- output 3: float32 [2048], P(('fit', 'pts'))
All inputs are finite; a program needn't handle non-finite values.
Results may differ from the reference program's by a relative error of at most 0.001.
Values are sent between devices in bfloat16 or wider.
A program may use at most 1 GiB of HBM per device.

```python
import jax
import jax.numpy as jnp
from jax import lax

N = 2048
K = 65536
D = 128
SWEEPS = 3
NUM_SRC = 16
ROW_BLOCK = 64

PRIOR_ALPHA = 1e-3
COUNT_EPS = 1e-6


def setup_inputs(seed: int = 0, part: int = 0) -> dict:
    root_key = jax.random.key(seed)
    part_key = jax.random.fold_in(root_key, part)
    key_cent, key_noise, key_assign, key_mnoise, key_logw = jax.random.split(part_key, 5)
    key_temp = jax.random.fold_in(root_key, 1000003)
    center_std = (2.0 / D ** 0.5) ** 0.5
    centers = center_std * jax.random.normal(key_cent, (NUM_SRC, D), jnp.float32)
    src_id = (jnp.arange(N, dtype=jnp.int32) * NUM_SRC) // N
    points = centers[src_id] + jax.random.normal(key_noise, (N, D), jnp.float32)
    assign = jax.random.randint(key_assign, (K,), 0, NUM_SRC)
    means_init = centers[assign] + 0.8 * jax.random.normal(key_mnoise, (K, D), jnp.float32)
    logw_init = jax.nn.log_softmax(0.5 * jax.random.normal(key_logw, (K,), jnp.float32))
    temp_steps = jax.random.uniform(key_temp, (SWEEPS,), jnp.float32)
    inv_temp = (0.25 + 0.2 * jnp.cumsum(temp_steps)) / D ** 0.5
    return {"points": points.astype(jnp.bfloat16), "means_init": means_init, "logw_init": logw_init, "inv_temp": inv_temp}


def em_sweep(points, mean_vecs, log_w, temp):
    mean_bf = mean_vecs.astype(jnp.bfloat16)
    mean_sq = jnp.sum(mean_vecs * mean_vecs, axis=1)
    row_blocks = points.reshape(N // ROW_BLOCK, ROW_BLOCK, D)

    def scan_body(state_pair, row_blk):
        counts, stat_sums = state_pair
        x_sq = jnp.sum(jnp.square(row_blk.astype(jnp.float32)), axis=1)
        cross_dot = jnp.dot(row_blk, mean_bf.T, preferred_element_type=jnp.float32)
        logits = log_w[None, :] - temp * (x_sq[:, None] - 2.0 * cross_dot + mean_sq[None, :])
        row_top = jnp.max(logits, axis=1)
        exp_total = jnp.sum(jnp.exp(logits - row_top[:, None]), axis=1)
        log_norm = row_top + jnp.log(exp_total)
        resp_prob = jnp.exp(logits - log_norm[:, None])
        counts = counts + jnp.sum(resp_prob, axis=0)
        stat_sums = stat_sums + jnp.dot(resp_prob.astype(jnp.bfloat16).T, row_blk, preferred_element_type=jnp.float32)
        return (counts, stat_sums), log_norm

    init_state = (jnp.zeros((K,), jnp.float32), jnp.zeros((K, D), jnp.float32))
    (counts, stat_sums), log_norm = lax.scan(scan_body, init_state, row_blocks)
    new_means = stat_sums / (counts[:, None] + COUNT_EPS)
    new_logw = jnp.log((counts + PRIOR_ALPHA) / (N + K * PRIOR_ALPHA))
    return new_means, new_logw, log_norm.reshape(N)


def reference(points, means_init, logw_init, inv_temp):
    mean_vecs = means_init
    log_w = logw_init
    log_norm = jnp.zeros((N,), jnp.float32)
    for sweep_idx in range(SWEEPS):
        mean_vecs, log_w, log_norm = em_sweep(points, mean_vecs, log_w, inv_temp[sweep_idx])
    return mean_vecs, log_w, log_norm
```

```python
import jax
import jax.numpy as jnp
from jax import lax
from jax.experimental import pallas as pl
from jax.experimental.pallas import tpu as pltpu
from jax.sharding import PartitionSpec as P

PRIOR_ALPHA = 1e-3
COUNT_EPS = 1e-6
LOG2E = 1.4426950408889634
LN2 = 0.6931471805599453
F32 = jnp.float32
BF16 = jnp.bfloat16
D = 128
KB = 1024
IT = 256
SUB = 64
VMEM = 60 * 2**20


def split3(v):
    hi = v.astype(BF16).astype(F32)
    mid = (v - hi).astype(BF16).astype(F32)
    return hi, mid, v - hi - mid


def lane_to_col(rows):
    r = rows.shape[0]
    eye = lax.broadcasted_iota(jnp.int32, (1, D, D), 1) == lax.broadcasted_iota(jnp.int32, (1, D, D), 2)
    col = jnp.sum(jnp.where(eye, rows[:, None, :], 0.0), axis=2, keepdims=True)
    return jnp.broadcast_to(col, (r, D, D)).reshape(r * D, D)


def col_to_lane(col):
    r = col.shape[0] // D
    eye = lax.broadcasted_iota(jnp.int32, (1, D, D), 1) == lax.broadcasted_iota(jnp.int32, (1, D, D), 2)
    return jnp.sum(jnp.where(eye, jnp.broadcast_to(col, (r * D, D)).reshape(r, D, D), 0.0), axis=1)


def aug_cols(c):
    lane = lax.broadcasted_iota(jnp.int32, c.shape, 1)
    hi, mid, lo = split3(c)
    v = jnp.where(lane == 0, hi, jnp.where(lane == 1, mid, lo))
    v = jnp.where(lane < 3, v, jnp.where(lane < 6, 1.0, 0.0))
    return v.astype(BF16)


def aug_rows(t):
    row = lax.broadcasted_iota(jnp.int32, (D, t.shape[1]), 0)
    hi, mid, lo = split3(-t)
    v = jnp.where(row == 3, hi, jnp.where(row == 4, mid, lo))
    v = jnp.where(row < 3, 1.0, jnp.where(row < 6, v, 0.0))
    return v.astype(BF16)


def fill_rhs(rhs_ref, xt_ref, g, t):
    rhs_ref[0:D, :] = (xt_ref[...].astype(F32) * g).astype(BF16)
    rhs_ref[D:, :] = aug_rows(t)


def e_block(lhs, rhs_ref, k1, m_ref, s_ref):
    n = rhs_ref.shape[1]
    kb = lhs.shape[0]
    for j in range(n // IT):
        sl = slice(j * IT, (j + 1) * IT)
        p = jnp.dot(lhs, rhs_ref[:, sl], preferred_element_type=F32)
        m = m_ref[:, sl]
        s = s_ref[:, sl]
        for r in range(0, kb, SUB):
            pr = p[r : r + SUB].reshape(SUB // 8, 8, IT)
            mn = jnp.maximum(m, jnp.max(pr, axis=0))
            e = jnp.sum(jnp.exp2((pr - mn[None]) * k1), axis=0)
            s = s * jnp.exp2((m - mn) * k1) + e
            m = mn
        m_ref[:, sl] = m
        s_ref[:, sl] = s


def m_block(lhs, rhs_ref, x_ref, k1):
    n = rhs_ref.shape[1]
    nacc = None
    ssum = None
    for j in range(n // IT):
        sl = slice(j * IT, (j + 1) * IT)
        p = jnp.dot(lhs, rhs_ref[:, sl], preferred_element_type=F32)
        r = jnp.exp2(p * k1)
        na = r[:, :D] + r[:, D:]
        nacc = na if nacc is None else nacc + na
        sj = jnp.dot(r.astype(BF16), x_ref[sl, :], preferred_element_type=F32)
        ssum = sj if ssum is None else ssum + sj
    cnt = jnp.sum(nacc, axis=1, keepdims=True)
    return ssum / (cnt + COUNT_EPS), cnt


def finish_stats(m_ref, s_ref, k1, out_ref):
    m = m_ref[...]
    top = jnp.max(m, axis=0, keepdims=True)
    tot = jnp.sum(s_ref[...] * jnp.exp2((m - top) * k1), axis=0, keepdims=True)
    out_ref[0:1, :] = top
    out_ref[1:2, :] = tot


def reset_stats(m_ref, s_ref):
    m_ref[...] = jnp.full(m_ref.shape, -jnp.inf, F32)
    s_ref[...] = jnp.zeros(s_ref.shape, F32)


def first_kernel(par_ref, mean_ref, logw_ref, xt_ref, lhs_ref, stat_ref, rhs_ref, m_ref, s_ref):
    step = pl.program_id(0)
    k1, gib, gh, g = par_ref[0, 0], par_ref[0, 1], par_ref[0, 2], par_ref[0, 3]

    @pl.when(step == 0)
    def _():
        reset_stats(m_ref, s_ref)
        fill_rhs(rhs_ref, xt_ref, g, jnp.zeros((1, rhs_ref.shape[1]), F32))

    mu = mean_ref[...]
    sq = jnp.sum(mu * mu, axis=1, keepdims=True)
    c = lane_to_col(logw_ref[...]) * gib - sq * gh
    lhs = jnp.concatenate([mu.astype(BF16), aug_cols(c)], axis=1)
    lhs_ref[...] = lhs
    e_block(lhs, rhs_ref, k1, m_ref, s_ref)

    @pl.when(step == pl.num_programs(0) - 1)
    def _():
        finish_stats(m_ref, s_ref, k1, stat_ref)


def make_mid_kernel(sweep, denom):
    def mid_kernel(par_ref, t_ref, lhs_ref, xt_ref, x_ref, new_ref, stat_ref, rhs_m, rhs_e, m_ref, s_ref):
        step = pl.program_id(0)
        k1 = par_ref[sweep, 0]
        k1n, gib, gh, gn = (par_ref[sweep + 1, i] for i in range(4))

        @pl.when(step == 0)
        def _():
            reset_stats(m_ref, s_ref)
            fill_rhs(rhs_m, xt_ref, par_ref[sweep, 3], t_ref[...])
            fill_rhs(rhs_e, xt_ref, gn, jnp.zeros((1, rhs_e.shape[1]), F32))

        mu, cnt = m_block(lhs_ref[...], rhs_m, x_ref, k1)
        logw = jnp.log((cnt + PRIOR_ALPHA) / denom)
        sq = jnp.sum(mu * mu, axis=1, keepdims=True)
        c = jnp.broadcast_to(logw * gib - sq * gh, mu.shape)
        lhs = jnp.concatenate([mu.astype(BF16), aug_cols(c)], axis=1)
        new_ref[...] = lhs
        e_block(lhs, rhs_e, k1n, m_ref, s_ref)

        @pl.when(step == pl.num_programs(0) - 1)
        def _():
            finish_stats(m_ref, s_ref, k1n, stat_ref)

    return mid_kernel


def make_last_kernel(sweep, denom):
    def last_kernel(par_ref, t_ref, lhs_ref, xt_ref, x_ref, mean_ref, logw_ref, rhs_m):
        k1 = par_ref[sweep, 0]

        @pl.when(pl.program_id(0) == 0)
        def _():
            fill_rhs(rhs_m, xt_ref, par_ref[sweep, 3], t_ref[...])

        mu, cnt = m_block(lhs_ref[...], rhs_m, x_ref, k1)
        mean_ref[...] = mu
        logw_ref[...] = jnp.log((col_to_lane(cnt) + PRIOR_ALPHA) / denom)

    return last_kernel


def solution(mesh):
    row_groups = mesh.shape["pts"]
    comp_groups = mesh.shape["comp"]

    def per_device(points, mean_vecs, log_w, inv_temp):
        n_loc = points.shape[0]
        n = n_loc * row_groups
        k_blk = mean_vecs.shape[0]
        k_total = k_blk * comp_groups
        kl = k_blk // row_groups
        sweeps = inv_temp.shape[0]
        denom = n + k_total * PRIOR_ALPHA
        nb = kl // KB
        p_idx = lax.axis_index("pts")
        x_sq = jnp.einsum("nd,nd->n", points, points, preferred_element_type=F32)
        x = lax.all_gather(points, "pts", tiled=True)
        xt = x.T
        mine = lax.dynamic_slice_in_dim(mean_vecs, p_idx * kl, kl, 0)
        logw = lax.dynamic_slice_in_dim(log_w, p_idx * kl, kl, 0).reshape(kl // D, D)
        g = jnp.where(inv_temp < 2.0**-60, 2.0**-60, jnp.where(inv_temp > 2.0**60, 2.0**60, 1.0)).astype(F32)
        k1 = (inv_temp / g) * (2.0 * LOG2E)
        par = jnp.stack([k1, g / inv_temp * 0.5, g * 0.5, g], axis=1)

        smem = pl.BlockSpec(memory_space=pltpu.SMEM)
        full = lambda s: pl.BlockSpec(s, lambda i: (0, 0))
        blk = lambda w: pl.BlockSpec((KB, w), lambda i: (i, 0))
        lane = pl.BlockSpec((KB // D, D), lambda i: (i, 0))
        rhs = pltpu.VMEM((2 * D, n), BF16)
        acc = pltpu.VMEM((8, n), F32)
        params = pltpu.CompilerParams(vmem_limit_bytes=VMEM)
        unit = 4 * n * kl * D
        lhs_s = jax.ShapeDtypeStruct((kl, 2 * D), BF16)
        stat_s = jax.ShapeDtypeStruct((2, n), F32)

        def cost(k):
            return pl.CostEstimate(flops=k * unit, bytes_accessed=8 * 2**20, transcendentals=n * kl)

        def shift(stat, sweep):
            st = lax.all_gather(stat, ("comp", "pts"))
            top = jnp.max(st[:, 0], axis=0)
            tot = jnp.sum(st[:, 1] * jnp.exp2((st[:, 0] - top) * k1[sweep]), axis=0)
            return (top + jnp.log2(tot) / k1[sweep])[None, :]

        lhs, stat = pl.pallas_call(
            first_kernel, grid=(nb,), name="first",
            out_shape=[lhs_s, stat_s],
            in_specs=[smem, blk(D), lane, full((D, n))],
            out_specs=[blk(2 * D), full((2, n))],
            scratch_shapes=[rhs, acc, acc],
            compiler_params=params, cost_estimate=cost(1),
        )(par, mine, logw, xt)
        for sweep in range(sweeps - 1):
            lhs, stat = pl.pallas_call(
                make_mid_kernel(sweep, denom), grid=(nb,), name="mid",
                out_shape=[lhs_s, stat_s],
                in_specs=[smem, full((1, n)), blk(2 * D), full((D, n)), full((n, D))],
                out_specs=[blk(2 * D), full((2, n))],
                scratch_shapes=[rhs, rhs, acc, acc],
                compiler_params=params, cost_estimate=cost(3),
            )(par, shift(stat, sweep), lhs, xt, x)
        t = shift(stat, sweeps - 1)
        means, logw = pl.pallas_call(
            make_last_kernel(sweeps - 1, denom), grid=(nb,), name="last",
            out_shape=[jax.ShapeDtypeStruct((kl, D), F32), jax.ShapeDtypeStruct((kl // D, D), F32)],
            in_specs=[smem, full((1, n)), blk(2 * D), full((D, n)), full((n, D))],
            out_specs=[blk(D), lane],
            scratch_shapes=[rhs],
            compiler_params=params, cost_estimate=cost(2),
        )(par, t, lhs, xt, x)
        means_out = lax.all_gather(means, "pts", tiled=True)
        logw_out = lax.all_gather(logw, "pts", tiled=True).reshape(k_blk)
        t_mine = lax.dynamic_slice_in_dim(t[0], p_idx * n_loc, n_loc, 0)
        lse = (LN2 * k1[sweeps - 1]) * t_mine - inv_temp[sweeps - 1] * x_sq
        return means_out, logw_out, lse

    row_spec = P(("fit", "pts"))
    comp_spec = P(("fit", "comp"))
    return jax.shard_map(
        per_device,
        mesh=mesh,
        in_specs=(P(("fit", "pts"), None), P(("fit", "comp"), None), comp_spec, P()),
        out_specs=(P(("fit", "comp"), None), comp_spec, row_spec),
        check_vma=False,
    )
```

```python
import jax
import jax.numpy as jnp
from jax import lax
from jax.experimental import pallas as pl
from jax.experimental.pallas import tpu as pltpu
from jax.sharding import PartitionSpec as P

PRIOR_ALPHA = 1e-3
COUNT_EPS = 1e-6
LOG2E = 1.4426950408889634
LN2 = 0.6931471805599453
F32 = jnp.float32
BF16 = jnp.bfloat16
D = 128
KB = 1024
IT = 256
SUB = 64
VMEM = 46 * 2**20
NPTS = 4
NDEV = 8
MESH = pl.DeviceIdType.MESH
FAR = 6
EARLY = 5


def split3(v):
    hi = v.astype(BF16).astype(F32)
    mid = (v - hi).astype(BF16).astype(F32)
    return hi, mid, v - hi - mid


def lane_to_col(rows):
    r = rows.shape[0]
    eye = lax.broadcasted_iota(jnp.int32, (1, D, D), 1) == lax.broadcasted_iota(jnp.int32, (1, D, D), 2)
    col = jnp.sum(jnp.where(eye, rows[:, None, :], 0.0), axis=2, keepdims=True)
    return jnp.broadcast_to(col, (r, D, D)).reshape(r * D, D)


def col_to_lane(col):
    r = col.shape[0] // D
    eye = lax.broadcasted_iota(jnp.int32, (1, D, D), 1) == lax.broadcasted_iota(jnp.int32, (1, D, D), 2)
    return jnp.sum(jnp.where(eye, jnp.broadcast_to(col, (r * D, D)).reshape(r, D, D), 0.0), axis=1)


def aug_cols(c):
    lane = lax.broadcasted_iota(jnp.int32, c.shape, 1)
    hi, mid, lo = split3(c)
    v = jnp.where(lane == 0, hi, jnp.where(lane == 1, mid, lo))
    v = jnp.where(lane < 3, v, jnp.where(lane < 6, 1.0, 0.0))
    return v.astype(BF16)


def aug_rows(t):
    row = lax.broadcasted_iota(jnp.int32, (D, t.shape[1]), 0)
    hi, mid, lo = split3(-t)
    v = jnp.where(row == 3, hi, jnp.where(row == 4, mid, lo))
    v = jnp.where(row < 3, 1.0, jnp.where(row < 6, v, 0.0))
    return v.astype(BF16)


def fill_rhs(rhs_ref, xt_ref, g, t):
    rhs_ref[0:D, :] = (xt_ref[...].astype(F32) * g).astype(BF16)
    rhs_ref[D:, :] = aug_rows(t)


def m_part(lhs, rhs_ref, x_ref, k1, j, nacc, ssum):
    sl = slice(j * IT, (j + 1) * IT)
    r = jnp.exp2(jnp.dot(lhs, rhs_ref[:, sl], preferred_element_type=F32) * k1)
    na = r[:, :D] + r[:, D:]
    sj = jnp.dot(r.astype(BF16), x_ref[sl, :], preferred_element_type=F32)
    return (na, sj) if nacc is None else (nacc + na, ssum + sj)


def m_block(lhs, rhs_ref, x_ref, k1):
    nacc = ssum = None
    for j in range(rhs_ref.shape[1] // IT):
        nacc, ssum = m_part(lhs, rhs_ref, x_ref, k1, j, nacc, ssum)
    return nacc, ssum


def e_part(lhs, rhs_ref, k1, j, m_ref, s_ref):
    sl = slice(j * IT, (j + 1) * IT)
    kb = lhs.shape[0]
    p = jnp.dot(lhs, rhs_ref[:, sl], preferred_element_type=F32)
    m = m_ref[:, sl]
    s = s_ref[:, sl]
    for r in range(0, kb, SUB):
        pr = p[r : r + SUB].reshape(SUB // 8, 8, IT)
        mn = jnp.maximum(m, jnp.max(pr, axis=0))
        e = jnp.sum(jnp.exp2((pr - mn[None]) * k1), axis=0)
        s = s * jnp.exp2((m - mn) * k1) + e
        m = mn
    m_ref[:, sl] = m
    s_ref[:, sl] = s


def reset_stats(m_ref, s_ref):
    m_ref[...] = jnp.full(m_ref.shape, -jnp.inf, F32)
    s_ref[...] = jnp.zeros(s_ref.shape, F32)


def make_kernel(denom, sweeps):
    def kernel(par_ref, pts_ref, mean_ref, logw_ref, out_ref, lw_out, lse_out,
               x_ref, xt_ref, rhs_m, rhs_e, a_ref, b_ref, mean_s, logw_s, mu_send, c_send, mu_far, c_far,
               m_ref, s_ref, s_s, n_s, aug, stat, gat,
               in_sem, xs, xr, ss, sr, bs, br, cs, cr, ds, dr, fs, fr, ws, wr, ls, lr):
        c = lax.axis_index("comp")
        p = lax.axis_index("pts")
        rows = pts_ref.shape[0]
        n = x_ref.shape[0]
        kl = b_ref.shape[0]
        nb = kl // KB
        nj = n // IT
        lb = KB // D
        q_far = lax.rem(p + 2, NPTS)
        q_sib = p + 1 - 2 * lax.rem(p, 2)
        q_dia = lax.rem(q_sib + 2, NPTS)
        sib, opp = {"pts": q_sib}, {"pts": q_far}
        me = c * NPTS + p
        others = []
        for off in range(1, NDEV):
            pos = lax.rem(me + off, NDEV)
            others.append((off, {"comp": pos // NPTS, "pts": lax.rem(pos, NPTS)}))

        def blk(base, i, size=KB):
            return pl.ds(pl.multiple_of(base + i * size, size), size)

        def remote(src, dst, send, recv, dev):
            return pltpu.make_async_remote_copy(src_ref=src, dst_ref=dst, send_sem=send, recv_sem=recv,
                                                device_id=dev, device_id_type=MESH)

        loads = [pltpu.make_async_copy(mean_ref.at[blk(p * kl, i)], mean_s.at[pl.ds(i * KB, KB)], in_sem.at[i])
                 for i in range(nb)]
        loads.append(pltpu.make_async_copy(logw_ref.at[blk(0, p, kl // D)], logw_s, in_sem.at[nb]))
        for cp in loads:
            cp.start()
        barrier = pltpu.get_barrier_semaphore()
        for _, dev in others:
            pl.semaphore_signal(barrier, inc=1, device_id=dev, device_id_type=MESH)
        pl.semaphore_wait(barrier, NDEV - 1)

        mine = blk(0, p, rows)
        xsend = [remote(pts_ref, x_ref.at[mine], xs.at[off], xr.at[off], {"pts": lax.rem(p + off, NPTS)})
                 for off in range(1, NPTS)]
        for cp in xsend:
            cp.start()
        x_ref[mine, :] = pts_ref[...]

        k1, gib, gh, g = (par_ref[0, i] for i in range(4))
        loads[nb].wait()

        def prep(i, carry):
            pltpu.make_async_copy(mean_ref.at[blk(p * kl, i)], mean_s.at[blk(0, i)], in_sem.at[i]).wait()
            mu = mean_s[blk(0, i), :]
            sq = jnp.sum(mu * mu, axis=1, keepdims=True)
            cc = lane_to_col(logw_s[blk(0, i, lb), :]) * gib - sq * gh
            a_ref[blk(0, i), :] = jnp.concatenate([mu.astype(BF16), aug_cols(cc)], axis=1)
            return carry

        lax.fori_loop(0, nb, prep, 0)
        for cp in xsend:
            cp.wait()
        xt_ref[...] = x_ref[...].astype(F32).T.astype(BF16)

        def exchange(rnd, k1, between=None):
            m = m_ref[...]
            top = jnp.max(m, axis=0, keepdims=True)
            stat[rnd, 0:1, :] = top
            stat[rnd, 1:2, :] = jnp.sum(s_ref[...] * jnp.exp2((m - top) * k1), axis=0, keepdims=True)
            sends = [remote(stat.at[rnd], gat.at[rnd, off], ss.at[rnd, off], sr.at[rnd, off], dev) for off, dev in others]
            for cp in sends:
                cp.start()
            if between is not None:
                between()
            for cp in sends:
                cp.wait()
            top = stat[rnd, 0:1, :]
            for off in range(1, NDEV):
                top = jnp.maximum(top, gat[rnd, off, 0:1, :])
            tot = stat[rnd, 1:2, :] * jnp.exp2((stat[rnd, 0:1, :] - top) * k1)
            for off in range(1, NDEV):
                tot += gat[rnd, off, 1:2, :] * jnp.exp2((gat[rnd, off, 0:1, :] - top) * k1)
            return top + jnp.log2(tot) / k1

        reset_stats(m_ref, s_ref)
        fill_rhs(rhs_e, xt_ref, g, jnp.zeros((1, n), F32))

        def e_step(i, carry):
            lhs = a_ref[blk(0, i), :]
            for j in range(nj):
                e_part(lhs, rhs_e, k1, j, m_ref, s_ref)
            return carry

        lax.fori_loop(0, nb, e_step, 0)
        t = exchange(0, k1)

        def bulk(i):
            return (remote(mu_send.at[blk(0, i)], mu_far.at[blk(0, i)], bs.at[i], br.at[i], opp),
                    remote(c_send.at[blk(0, i, lb)], c_far.at[blk(0, i, lb)], cs.at[i], cr.at[i], opp))

        for sweep in range(sweeps - 1):
            src, dst = (a_ref, b_ref) if sweep % 2 == 0 else (b_ref, a_ref)
            share = sweep == sweeps - 2
            k1 = par_ref[sweep, 0]
            k1n, gib, gh, gn = (par_ref[sweep + 1, i] for i in range(4))
            fill_rhs(rhs_m, xt_ref, par_ref[sweep, 3], t)
            fill_rhs(rhs_e, xt_ref, gn, jnp.zeros((1, n), F32))
            reset_stats(m_ref, s_ref)

            def epilogue(i, dst=dst, share=share, gib=gib, gh=gh):
                cnt = jnp.sum(n_s[...], axis=1, keepdims=True)
                mu = s_s[...] / (cnt + COUNT_EPS)
                logw = jnp.log((cnt + PRIOR_ALPHA) / denom)
                sq = jnp.sum(mu * mu, axis=1, keepdims=True)
                cc = jnp.broadcast_to(logw * gib - sq * gh, mu.shape)
                mu_bf = mu.astype(BF16)
                aug[...] = jnp.concatenate([mu_bf, aug_cols(cc)], axis=1)
                dst[blk(0, i), :] = aug[...]
                if share:
                    mu_send[blk(0, i), :] = mu_bf
                    c_send[blk(0, i, lb), :] = col_to_lane(cc)

            n_s[...], s_s[...] = m_block(src[0:KB, :], rhs_m, x_ref, k1)

            def mid_step(i, carry, src=src, share=share, k1=k1, k1n=k1n, epilogue=epilogue):
                lhs = src[blk(0, i), :]
                nacc, ssum = m_part(lhs, rhs_m, x_ref, k1, 0, None, None)
                epilogue(i - 1)
                for j in range(1, nj):
                    nacc, ssum = m_part(lhs, rhs_m, x_ref, k1, j, nacc, ssum)
                    e_part(aug[...], rhs_e, k1n, j - 1, m_ref, s_ref)
                e_part(aug[...], rhs_e, k1n, nj - 1, m_ref, s_ref)
                n_s[...] = nacc
                s_s[...] = ssum
                if share:
                    @pl.when(i - 1 < EARLY)
                    def _():
                        for cp in bulk(i - 1):
                            cp.start()
                return carry

            lax.fori_loop(1, nb, mid_step, 0)
            epilogue(nb - 1)
            for j in range(nj):
                e_part(aug[...], rhs_e, k1n, j, m_ref, s_ref)

            def rest():
                for i in range(EARLY, FAR):
                    for cp in bulk(i):
                        cp.start()

            t = exchange(sweep + 1, k1n, rest if share else None)

        k1, beta, g = par_ref[sweeps - 1, 0], par_ref[sweeps - 1, 4], par_ref[sweeps - 1, 3]
        fill_rhs(rhs_m, xt_ref, g, t)
        stat[0, 0:1, :] = t
        own = pl.ds(pl.multiple_of(p * rows, rows), rows)
        xo = xt_ref[:, own].astype(F32)
        lse_out[...] = (LN2 * k1) * stat[0, 0:1, own] - beta * jnp.sum(xo * xo, axis=0, keepdims=True)

        late = nb - FAR

        def place(i, near_q, far_q):
            near = lax.rem(i + FAR, nb)
            return jnp.where(i < nb, near_q * nb + near, far_q * nb + i - nb)

        def to_sib(i, own_side=True):
            pos = place(i, p, q_far) if own_side else place(i, q_sib, q_dia)
            return remote(out_ref.at[blk(0, pos)], out_ref.at[blk(0, pos)], ds.at[i], dr.at[i], sib)

        def to_opp(i, q=None):
            rows_ = out_ref.at[blk(0, (p if q is None else q) * nb + FAR + i)]
            return remote(rows_, rows_, fs.at[i], fr.at[i], opp)

        def forward(i, q=None):
            rows_ = out_ref.at[blk(0, (q_far if q is None else q) * nb + FAR + i)]
            return remote(rows_, rows_, ws.at[i], wr.at[i], sib)

        def lw(k, q, first, count, dev):
            r_ = lw_out.at[pl.ds(pl.multiple_of((q * nb + first) * lb, lb), count * lb)]
            return remote(r_, r_, ls.at[k], lr.at[k], dev)

        def last_step(i, carry):
            pos_l = jnp.where(i < nb, lax.rem(i + FAR, nb), i)
            pos = place(i, p, q_far)
            nacc, ssum = m_block(a_ref[blk(0, pos_l), :], rhs_m, x_ref, k1)
            cnt = jnp.sum(nacc, axis=1, keepdims=True)
            out_ref[blk(0, pos), :] = ssum / (cnt + COUNT_EPS)
            lw_out[blk(0, pos, lb), :] = jnp.log((col_to_lane(cnt) + PRIOR_ALPHA) / denom)

            @pl.when(i < FAR)
            def _():
                for cp in bulk(i):
                    cp.wait()
                a_ref[blk(kl, i), :] = jnp.concatenate(
                    [mu_far[blk(0, i), :], aug_cols(lane_to_col(c_far[blk(0, i, lb), :]))], axis=1)

            to_sib(i).start()

            @pl.when(i < late)
            def _():
                to_opp(i).start()

            @pl.when(i == late)
            def _():
                lw(0, p, FAR, late, opp).start()

            @pl.when(i == nb)
            def _():
                lw(1, p, 0, nb, sib).start()

            for k in range(late):
                @pl.when(i == nb + FAR - 2 * (late - k))
                def _(k=k):
                    to_opp(k, q_far).wait_recv()
                    forward(k).start()
            return carry

        steps = nb + FAR
        lax.fori_loop(0, steps, last_step, 0)
        lw(2, q_far, 0, FAR, sib).start()
        lw(0, q_far, FAR, late, opp).wait_recv()
        lw(3, q_far, FAR, late, sib).start()

        def drain(i, carry):
            to_sib(i).wait_send()
            to_sib(i, False).wait_recv()
            return carry

        lax.fori_loop(0, steps, drain, 0)
        for k in range(late):
            to_opp(k).wait_send()
            forward(k).wait_send()
            forward(k, q_dia).wait_recv()
        lw(0, p, FAR, late, opp).wait_send()
        lw(1, p, 0, nb, sib).wait_send()
        lw(1, q_sib, 0, nb, sib).wait_recv()
        lw(2, q_far, 0, FAR, sib).wait_send()
        lw(2, q_dia, 0, FAR, sib).wait_recv()
        lw(3, q_far, FAR, late, sib).wait_send()
        lw(3, q_dia, FAR, late, sib).wait_recv()

    return kernel


def solution(mesh):
    row_groups = mesh.shape["pts"]
    comp_groups = mesh.shape["comp"]

    def per_device(points, mean_vecs, log_w, inv_temp):
        n_loc = points.shape[0]
        n = n_loc * row_groups
        k_blk = mean_vecs.shape[0]
        k_total = k_blk * comp_groups
        kl = k_blk // row_groups
        nb = kl // KB
        late = nb - FAR
        sweeps = inv_temp.shape[0]
        denom = n + k_total * PRIOR_ALPHA
        g = jnp.where(inv_temp < 2.0**-60, 2.0**-60, jnp.where(inv_temp > 2.0**60, 2.0**60, 1.0)).astype(F32)
        k1 = (inv_temp / g) * (2.0 * LOG2E)
        par = jnp.stack([k1, g / inv_temp * 0.5, g * 0.5, g, inv_temp], axis=1)
        vm = pltpu.VMEM
        dma = lambda *s: pltpu.SemaphoreType.DMA(s)
        anyspace = pl.BlockSpec(memory_space=pl.ANY)
        vspec = pl.BlockSpec(memory_space=pltpu.VMEM)
        means, logw, lse = pl.pallas_call(
            make_kernel(denom, sweeps), name="em",
            out_shape=[vm((k_blk, D), F32), vm((k_blk // D, D), F32), vm((1, n_loc), F32)],
            in_specs=[pl.BlockSpec(memory_space=pltpu.SMEM), vspec, anyspace, anyspace],
            out_specs=[vspec, vspec, vspec],
            scratch_shapes=[
                vm((n, D), BF16), vm((D, n), BF16), vm((2 * D, n), BF16), vm((2 * D, n), BF16),
                vm((kl + FAR * KB, 2 * D), BF16), vm((kl, 2 * D), BF16), vm((kl, D), F32), vm((kl // D, D), F32),
                vm((kl, D), BF16), vm((kl // D, D), F32), vm((FAR * KB, D), BF16), vm((FAR * KB // D, D), F32),
                vm((8, n), F32), vm((8, n), F32), vm((KB, D), F32), vm((KB, D), F32), vm((KB, 2 * D), BF16),
                vm((sweeps, 2, n), F32), vm((sweeps, NDEV, 2, n), F32),
                dma(nb + 1), dma(NPTS), dma(NPTS), dma(sweeps, NDEV), dma(sweeps, NDEV),
                dma(FAR), dma(FAR), dma(FAR), dma(FAR), dma(nb + FAR), dma(nb + FAR), dma(late), dma(late),
                dma(late), dma(late), dma(4), dma(4)],
            compiler_params=pltpu.CompilerParams(collective_id=0, has_side_effects=True, vmem_limit_bytes=VMEM),
        )(par, points, mean_vecs, log_w.reshape(k_blk // D, D))
        return means, logw.reshape(k_blk), lse.reshape(n_loc)

    row_spec = P(("fit", "pts"))
    comp_spec = P(("fit", "comp"))
    return jax.shard_map(
        per_device,
        mesh=mesh,
        in_specs=(P(("fit", "pts"), None), P(("fit", "comp"), None), comp_spec, P()),
        out_specs=(P(("fit", "comp"), None), comp_spec, row_spec),
        check_vma=False,
    )
```

```python
import functools

import jax
import jax.numpy as jnp
from jax import lax
from jax.experimental import pallas as pl
from jax.experimental.pallas import tpu as pltpu
from jax.sharding import PartitionSpec as P

PRIOR_ALPHA = 1e-3
COUNT_EPS = 1e-6
LOG2E = 1.4426950408889634
LN2 = 0.6931471805599453
F32 = jnp.float32
BF16 = jnp.bfloat16
D = 128
KB = 1024
IT = 256
SUB = 64
VMEM = 46 * 2**20
NPTS = 4
NDEV = 8
MESH = pl.DeviceIdType.MESH
FAR = 6
EARLY = 4


def split3(v):
    hi = v.astype(BF16).astype(F32)
    mid = (v - hi).astype(BF16).astype(F32)
    return hi, mid, v - hi - mid


def lane_to_col(rows):
    r = rows.shape[0]
    eye = lax.broadcasted_iota(jnp.int32, (1, D, D), 1) == lax.broadcasted_iota(jnp.int32, (1, D, D), 2)
    col = jnp.sum(jnp.where(eye, rows[:, None, :], 0.0), axis=2, keepdims=True)
    return jnp.broadcast_to(col, (r, D, D)).reshape(r * D, D)


def col_to_lane(col):
    r = col.shape[0] // D
    eye = lax.broadcasted_iota(jnp.int32, (1, D, D), 1) == lax.broadcasted_iota(jnp.int32, (1, D, D), 2)
    return jnp.sum(jnp.where(eye, jnp.broadcast_to(col, (r * D, D)).reshape(r, D, D), 0.0), axis=1)


def aug_cols(c):
    lane = lax.broadcasted_iota(jnp.int32, c.shape, 1)
    hi, mid, lo = split3(c)
    v = jnp.where(lane == 0, hi, jnp.where(lane == 1, mid, lo))
    v = jnp.where(lane < 3, v, jnp.where(lane < 6, 1.0, 0.0))
    return v.astype(BF16)


def aug_rows(t):
    row = lax.broadcasted_iota(jnp.int32, (D, t.shape[1]), 0)
    hi, mid, lo = split3(-t)
    v = jnp.where(row == 3, hi, jnp.where(row == 4, mid, lo))
    v = jnp.where(row < 3, 1.0, jnp.where(row < 6, v, 0.0))
    return v.astype(BF16)


def fill_rhs(rhs_ref, xt_ref, g, t):
    rhs_ref[0:D, :] = (xt_ref[...].astype(F32) * g).astype(BF16)
    rhs_ref[D:, :] = aug_rows(t)


def m_part(lhs, rhs_ref, x_ref, k1, j, nacc, ssum):
    sl = slice(j * IT, (j + 1) * IT)
    r = jnp.exp2(jnp.dot(lhs, rhs_ref[:, sl], preferred_element_type=F32) * k1)
    na = r[:, :D] + r[:, D:]
    sj = jnp.dot(r.astype(BF16), x_ref[sl, :], preferred_element_type=F32)
    return (na, sj) if nacc is None else (nacc + na, ssum + sj)


def m_block(lhs, rhs_ref, x_ref, k1):
    nacc = ssum = None
    for j in range(rhs_ref.shape[1] // IT):
        nacc, ssum = m_part(lhs, rhs_ref, x_ref, k1, j, nacc, ssum)
    return nacc, ssum


def m_block_known(p_ref, rows, t_ref, x_ref, k1):
    nacc = ssum = None
    for j in range(t_ref.shape[1] // IT):
        sl = slice(j * IT, (j + 1) * IT)
        p = p_ref[rows, sl]
        r = jnp.exp2((p.reshape(p.shape[0] // 8, 8, IT) - t_ref[:, sl][None]) * k1).reshape(p.shape)
        na = r[:, :D] + r[:, D:]
        sj = jnp.dot(r.astype(BF16), x_ref[sl, :], preferred_element_type=F32)
        nacc, ssum = (na, sj) if nacc is None else (nacc + na, ssum + sj)
    return nacc, ssum


def e_part(lhs, rhs_ref, k1, j, m_ref, s_ref, base=None):
    sl = slice(j * IT, (j + 1) * IT) if base is None else pl.ds(pl.multiple_of(base + j * IT, IT), IT)
    kb = lhs.shape[0]
    p = jnp.dot(lhs, rhs_ref[:, sl], preferred_element_type=F32)
    m = m_ref[:, sl]
    s = s_ref[:, sl]
    for r in range(0, kb, SUB):
        pr = p[r : r + SUB].reshape(SUB // 8, 8, IT)
        mn = jnp.maximum(m, jnp.max(pr, axis=0))
        e = jnp.sum(jnp.exp2((pr - mn[None]) * k1), axis=0)
        s = s * jnp.exp2((m - mn) * k1) + e
        m = mn
    m_ref[:, sl] = m
    s_ref[:, sl] = s


def reset_stats(m_ref, s_ref):
    m_ref[...] = jnp.full(m_ref.shape, -jnp.inf, F32)
    s_ref[...] = jnp.zeros(s_ref.shape, F32)


def sweep_scalars(beta):
    small, large = beta < 2.0**-60, beta > 2.0**60
    g = jnp.where(small, 2.0**-60, jnp.where(large, 2.0**60, 1.0))
    g_inv = jnp.where(small, 2.0**60, jnp.where(large, 2.0**-60, 1.0))
    return (beta * g_inv) * (2.0 * LOG2E), g / beta * 0.5, g * 0.5, g


def make_kernel(denom, sweeps):
    def kernel(par_ref, pts_ref, mean_ref, logw_ref, out_ref, lw_out, lse_out,
               x_ref, xt_ref, rhs_m, rhs_e, a_ref, b_ref, logw_s, mu_send, c_send, mu_far, c_far,
               m_ref, s_ref, s_s, n_s, aug, stat, gat, p_ref, t_ref,
               in_sem, xs, xr, ss, sr, bs, br, cs, cr, ds, dr, fs, fr, ws, wr, ls, lr):
        c = lax.axis_index("comp")
        p = lax.axis_index("pts")
        rows = pts_ref.shape[0]
        n = x_ref.shape[0]
        kl = b_ref.shape[0]
        nb = kl // KB
        nj = n // IT
        lb = KB // D
        q_far = lax.rem(p + 2, NPTS)
        q_sib = p + 1 - 2 * lax.rem(p, 2)
        q_dia = lax.rem(q_sib + 2, NPTS)
        sib, opp = {"pts": q_sib}, {"pts": q_far}
        me = c * NPTS + p
        others = []
        for off in range(1, NDEV):
            pos = lax.rem(me + off, NDEV)
            others.append((off, {"comp": pos // NPTS, "pts": lax.rem(pos, NPTS)}))

        def blk(base, i, size=KB):
            return pl.ds(pl.multiple_of(base + i * size, size), size)

        def remote(src, dst, send, recv, dev):
            return pltpu.make_async_remote_copy(src_ref=src, dst_ref=dst, send_sem=send, recv_sem=recv,
                                                device_id=dev, device_id_type=MESH)

        loads = [pltpu.make_async_copy(mean_ref.at[blk(p * kl, i)], out_ref.at[blk(p * kl, i)], in_sem.at[i])
                 for i in range(nb)]
        loads.append(pltpu.make_async_copy(logw_ref.at[blk(0, p, kl // D)], logw_s, in_sem.at[nb]))
        for cp in loads:
            cp.start()
        barrier = pltpu.get_barrier_semaphore()
        for _, dev in others:
            pl.semaphore_signal(barrier, inc=1, device_id=dev, device_id_type=MESH)
        k1, gib, gh, g = sweep_scalars(par_ref[0])
        loads[nb].wait()

        def prep(i, carry):
            pltpu.make_async_copy(mean_ref.at[blk(p * kl, i)], out_ref.at[blk(p * kl, i)], in_sem.at[i]).wait()
            mu = out_ref[blk(p * kl, i), :]
            sq = jnp.sum(mu * mu, axis=1, keepdims=True)
            cc = lane_to_col(logw_s[blk(0, i, lb), :]) * gib - sq * gh
            a_ref[blk(0, i), :] = jnp.concatenate([mu.astype(BF16), aug_cols(cc)], axis=1)
            return carry

        mine = blk(0, p, rows)
        theirs = blk(0, q_far, rows)
        x_ref[mine, :] = pts_ref[...]
        rhs_e[D:, :] = aug_rows(jnp.zeros((1, n), F32))
        reset_stats(m_ref, s_ref)
        ahead = nb // 2
        lax.fori_loop(0, ahead, prep, 0)
        pl.semaphore_wait(barrier, NDEV - 1)
        x_opp = remote(pts_ref, x_ref.at[mine], xs.at[0], xr.at[0], opp)
        x_sib = remote(pts_ref, x_ref.at[mine], xs.at[1], xr.at[1], sib)
        x_fwd = remote(x_ref.at[theirs], x_ref.at[theirs], xs.at[2], xr.at[2], sib)
        x_sib.start()
        x_opp.start()
        lax.fori_loop(ahead, nb, prep, 0)

        half = n // 2

        def columns(base):
            cols = pl.ds(pl.multiple_of(base, half), half)
            xt = x_ref[cols, :].astype(F32).T
            xt_ref[:, cols] = xt.astype(BF16)
            rhs_e[0:D, cols] = (xt * g).astype(BF16)

        near_cols = (p // 2) * half
        far_cols = half - near_cols
        per = nb // 2

        def e_step(i, carry):
            @pl.when(i == per // 2)
            def _():
                x_opp.wait()
                x_fwd.start()

            @pl.when(i == per)
            def _():
                x_fwd.wait()
                columns(far_cols)

            base = jnp.where(i < per, near_cols, far_cols)
            lhs = a_ref[blk(0, lax.rem(i, per), 2 * KB), :]
            for j in range(nj // 2):
                e_part(lhs, rhs_e, k1, j, m_ref, s_ref, base)
            return carry

        x_sib.wait()
        columns(near_cols)
        lax.fori_loop(0, nb, e_step, 0)

        def exchange(rnd, k1, between):
            m = m_ref[...]
            top = jnp.max(m, axis=0, keepdims=True)
            tot = jnp.sum(s_ref[...] * jnp.exp2((m - top) * k1), axis=0, keepdims=True)
            stat[rnd] = top + jnp.log2(tot) / k1
            sends = [remote(stat.at[rnd], gat.at[rnd, off], ss.at[rnd, off], sr.at[rnd, off], dev) for off, dev in others]
            for cp in sends:
                cp.start()
            between()
            for cp in sends:
                cp.wait()
            parts = [stat[rnd]] + [gat[rnd, off] for off in range(1, NDEV)]
            top = parts[0]
            for v in parts[1:]:
                top = jnp.maximum(top, v)
            tot = jnp.exp2((parts[0] - top) * k1)
            for v in parts[1:]:
                tot += jnp.exp2((v - top) * k1)
            t = top + jnp.log2(tot) / k1
            t_ref[...] = jnp.broadcast_to(t, t_ref.shape)
            return t

        def products(src, first, count):
            wide = n // 4

            def step(i, carry):
                rows_ = i // 4
                cols = pl.ds(pl.multiple_of(lax.rem(i, 4) * wide, wide), wide)
                p_ref[blk(0, rows_), cols] = jnp.dot(
                    src[blk(first * KB, rows_), :], rhs_e[:, cols], preferred_element_type=F32)
                return carry

            lax.fori_loop(0, 4 * count, step, 0)

        t = exchange(0, k1, lambda: products(a_ref, 0, 1))

        def bulk(i):
            return (remote(mu_send.at[blk(0, i)], mu_far.at[blk(0, i)], bs.at[i], br.at[i], opp),
                    remote(c_send.at[blk(0, i, lb)], c_far.at[blk(0, i, lb)], cs.at[i], cr.at[i], opp))

        for sweep in range(sweeps - 1):
            src, dst = (a_ref, b_ref) if sweep % 2 == 0 else (b_ref, a_ref)
            share = sweep == sweeps - 2
            k1, _, _, g = sweep_scalars(par_ref[sweep])
            k1n, gib, gh, gn = sweep_scalars(par_ref[sweep + 1])
            fill_rhs(rhs_m, xt_ref, g, t)
            fill_rhs(rhs_e, xt_ref, gn, jnp.zeros((1, n), F32))
            reset_stats(m_ref, s_ref)

            def epilogue(i, dst=dst, share=share, gib=gib, gh=gh):
                cnt = jnp.sum(n_s[...], axis=1, keepdims=True)
                mu = s_s[...] / (cnt + COUNT_EPS)
                logw = jnp.log((cnt + PRIOR_ALPHA) / denom)
                sq = jnp.sum(mu * mu, axis=1, keepdims=True)
                cc = jnp.broadcast_to(logw * gib - sq * gh, mu.shape)
                mu_bf = mu.astype(BF16)
                aug[...] = jnp.concatenate([mu_bf, aug_cols(cc)], axis=1)
                dst[blk(0, i), :] = aug[...]
                if share:
                    mu_send[blk(0, i), :] = mu_bf
                    c_send[blk(0, i, lb), :] = col_to_lane(cc)

            n_s[...], s_s[...] = m_block_known(p_ref, slice(0, KB), t_ref, x_ref, k1)

            def mid_step(i, carry, src=src, share=share, k1=k1, k1n=k1n, epilogue=epilogue):
                lhs = src[blk(0, i), :]
                nacc, ssum = m_part(lhs, rhs_m, x_ref, k1, 0, None, None)
                epilogue(i - 1)
                for j in range(1, nj):
                    nacc, ssum = m_part(lhs, rhs_m, x_ref, k1, j, nacc, ssum)
                    e_part(aug[...], rhs_e, k1n, j - 1, m_ref, s_ref)
                e_part(aug[...], rhs_e, k1n, nj - 1, m_ref, s_ref)
                n_s[...] = nacc
                s_s[...] = ssum
                if share:
                    @pl.when(i - 1 < EARLY)
                    def _():
                        for cp in bulk(i - 1):
                            cp.start()
                return carry

            lax.fori_loop(1, nb, mid_step, 0)
            epilogue(nb - 1)
            for j in range(nj):
                e_part(aug[...], rhs_e, k1n, j, m_ref, s_ref)

            def meanwhile(dst=dst, share=share):
                if share:
                    for i in range(EARLY, FAR):
                        for cp in bulk(i):
                            cp.start()
                    products(dst, FAR, nb - FAR)
                else:
                    products(dst, 0, 1)

            t = exchange(sweep + 1, k1n, meanwhile)

        beta = par_ref[sweeps - 1]
        k1, _, _, g = sweep_scalars(beta)
        fill_rhs(rhs_m, xt_ref, g, t)
        stat[0] = t
        own = pl.ds(pl.multiple_of(p * rows, rows), rows)
        xo = xt_ref[:, own].astype(F32)
        lse_out[...] = (LN2 * k1) * stat[0, 0:1, own] - beta * jnp.sum(xo * xo, axis=0, keepdims=True)

        late = nb - FAR

        def place(i, near_q, far_q):
            near = lax.rem(i + FAR, nb)
            return jnp.where(i < nb, near_q * nb + near, far_q * nb + i - nb)

        def to_sib(i, own_side=True):
            pos = place(i, p, q_far) if own_side else place(i, q_sib, q_dia)
            return remote(out_ref.at[blk(0, pos)], out_ref.at[blk(0, pos)], ds.at[i], dr.at[i], sib)

        def to_opp(i, q=None):
            rows_ = out_ref.at[blk(0, (p if q is None else q) * nb + FAR + i)]
            return remote(rows_, rows_, fs.at[i], fr.at[i], opp)

        def forward(i, q=None):
            rows_ = out_ref.at[blk(0, (q_far if q is None else q) * nb + FAR + i)]
            return remote(rows_, rows_, ws.at[i], wr.at[i], sib)

        def lw(k, q, first, count, dev):
            r_ = lw_out.at[pl.ds(pl.multiple_of((q * nb + first) * lb, lb), count * lb)]
            return remote(r_, r_, ls.at[k], lr.at[k], dev)

        def last_step(i, carry, known=False):
            pos_l = jnp.where(i < nb, lax.rem(i + FAR, nb), i)
            pos = place(i, p, q_far)
            conv = jnp.minimum(i, FAR - 1)

            @pl.when(i < FAR)
            def _():
                for cp in bulk(i):
                    cp.wait()

            if known:
                nacc, ssum = m_block_known(p_ref, blk(0, i), t_ref, x_ref, k1)
            else:
                nacc, ssum = m_block(a_ref[blk(0, pos_l), :], rhs_m, x_ref, k1)
            a_ref[blk(kl, conv), :] = jnp.concatenate(
                [mu_far[blk(0, conv), :], aug_cols(lane_to_col(c_far[blk(0, conv, lb), :]))], axis=1)
            cnt = jnp.sum(nacc, axis=1, keepdims=True)
            out_ref[blk(0, pos), :] = ssum / (cnt + COUNT_EPS)
            lw_out[blk(0, pos, lb), :] = jnp.log((col_to_lane(cnt) + PRIOR_ALPHA) / denom)

            to_sib(i).start()

            @pl.when(i < late)
            def _():
                to_opp(i).start()

            @pl.when(i == late)
            def _():
                lw(0, p, FAR, late, opp).start()

            @pl.when(i == nb)
            def _():
                lw(1, p, 0, nb, sib).start()

            for k in range(late):
                @pl.when(i == nb + FAR - 2 * (late - k))
                def _(k=k):
                    to_opp(k, q_far).wait_recv()
                    forward(k).start()
            return carry

        steps = nb + FAR
        lax.fori_loop(0, late, functools.partial(last_step, known=True), 0)
        lax.fori_loop(late, steps, last_step, 0)
        lw(2, q_far, 0, FAR, sib).start()
        lw(0, q_far, FAR, late, opp).wait_recv()
        lw(3, q_far, FAR, late, sib).start()

        def drain(i, carry):
            to_sib(i).wait_send()
            to_sib(i, False).wait_recv()
            return carry

        lax.fori_loop(0, steps, drain, 0)
        for k in range(late):
            to_opp(k).wait_send()
            forward(k).wait_send()
            forward(k, q_dia).wait_recv()
        lw(0, p, FAR, late, opp).wait_send()
        lw(1, p, 0, nb, sib).wait_send()
        lw(1, q_sib, 0, nb, sib).wait_recv()
        lw(2, q_far, 0, FAR, sib).wait_send()
        lw(2, q_dia, 0, FAR, sib).wait_recv()
        lw(3, q_far, FAR, late, sib).wait_send()
        lw(3, q_dia, FAR, late, sib).wait_recv()

    return kernel


def solution(mesh):
    row_groups = mesh.shape["pts"]
    comp_groups = mesh.shape["comp"]

    def per_device(points, mean_vecs, log_w, inv_temp):
        n_loc = points.shape[0]
        n = n_loc * row_groups
        k_blk = mean_vecs.shape[0]
        k_total = k_blk * comp_groups
        kl = k_blk // row_groups
        nb = kl // KB
        late = nb - FAR
        sweeps = inv_temp.shape[0]
        denom = n + k_total * PRIOR_ALPHA
        vm = pltpu.VMEM
        dma = lambda *s: pltpu.SemaphoreType.DMA(s)
        anyspace = pl.BlockSpec(memory_space=pl.ANY)
        vspec = pl.BlockSpec(memory_space=pltpu.VMEM)
        means, logw, lse = pl.pallas_call(
            make_kernel(denom, sweeps), name="em",
            out_shape=[vm((k_blk, D), F32), vm((k_blk // D, D), F32), vm((1, n_loc), F32)],
            in_specs=[pl.BlockSpec(memory_space=pltpu.SMEM), vspec, anyspace, anyspace],
            out_specs=[vspec, vspec, vspec],
            scratch_shapes=[
                vm((n, D), BF16), vm((D, n), BF16), vm((2 * D, n), BF16), vm((2 * D, n), BF16),
                vm((kl + FAR * KB, 2 * D), BF16), vm((kl, 2 * D), BF16), vm((kl // D, D), F32),
                vm((kl, D), BF16), vm((kl // D, D), F32), vm((FAR * KB, D), BF16), vm((FAR * KB // D, D), F32),
                vm((8, n), F32), vm((8, n), F32), vm((KB, D), F32), vm((KB, D), F32), vm((KB, 2 * D), BF16),
                vm((sweeps, 1, n), F32), vm((sweeps, NDEV, 1, n), F32), vm((late * KB, n), F32), vm((8, n), F32),
                dma(nb + 1), dma(NPTS), dma(NPTS), dma(sweeps, NDEV), dma(sweeps, NDEV),
                dma(FAR), dma(FAR), dma(FAR), dma(FAR), dma(nb + FAR), dma(nb + FAR), dma(late), dma(late),
                dma(late), dma(late), dma(4), dma(4)],
            compiler_params=pltpu.CompilerParams(collective_id=0, has_side_effects=True, vmem_limit_bytes=VMEM),
        )(inv_temp, points, mean_vecs, log_w.reshape(k_blk // D, D))
        return means, logw.reshape(k_blk), lse.reshape(n_loc)

    row_spec = P(("fit", "pts"))
    comp_spec = P(("fit", "comp"))
    return jax.shard_map(
        per_device,
        mesh=mesh,
        in_specs=(P(("fit", "pts"), None), P(("fit", "comp"), None), comp_spec, P()),
        out_specs=(P(("fit", "comp"), None), comp_spec, row_spec),
        check_vma=False,
    )
```
